32 devices in a mesh: pa: 32 (over z, y, x, core).
Axes of the slice: x: 2, y: 2, z: 4, core: 2. Of those that a mesh axis runs over, the one named last changes fastest.
Arguments:
- image_real: float32 [8, 4096, 4096], P(None, 'pa'), may hold values from -6 to 6
- image_imag: float32 [8, 4096, 4096], P(None, 'pa'), may hold values from -6 to 6
Outputs:
- spectrum_real: float32 [8, 4096, 4096], P(None, 'pa')
- spectrum_imag: float32 [8, 4096, 4096], P(None, 'pa')
The draws below stay inside these ranges and needn't reach their ends.
All inputs are finite; a program needn't handle non-finite values.
Results may differ from the reference program's by a relative error of at most 0.0003.
Values sent between devices are 32-bit elements.
A program may use at most 256 MiB of HBM per device.

```python
import math
import jax
import jax.numpy as jnp
from jax import lax

N = 4096
FRAMES = 8


def levels(rng, dims, cuts, least, high):
    def one(position, shards_of):
        draws = jax.random.uniform(jax.random.fold_in(jax.random.fold_in(rng, 6), position), (shards_of,), jnp.float32, least / len(cuts), high / len(cuts))
        return jnp.repeat(jnp.exp(draws), dims[position] // shards_of).reshape((-1,) + (1,) * (len(dims) - position - 1))

    factor_of = one(*cuts[0])
    for cut in cuts[1:]:
        factor_of = factor_of * one(*cut)
    return factor_of


def gaussian(key, shape, width, most, shards=(), held_as=jnp.bfloat16):
    gain = levels(key, shape, shards, -0.22, 0.18) if shards else 1.0
    result = jax.random.normal(key, shape, jnp.float32) * width * gain
    return jnp.minimum(jnp.maximum(result, -most), most).astype(held_as)


def setup_inputs(seed: int = 0) -> dict:
    key_of = jax.random.split(jax.random.key(seed), 3)
    image_real = gaussian(key_of[0], (FRAMES, N, N), 1.0, 6.0, ((1, 32),), jnp.float32)
    image_imag = gaussian(key_of[1], (FRAMES, N, N), 1.0, 6.0, ((1, 32),), jnp.float32)
    return {"image_real": image_real, "image_imag": image_imag}


canceller_gain = 1.0 / math.sqrt(6.0)

def hamming(offset, sample_count, length):
    sample_index = (offset + jnp.arange(sample_count, dtype=jnp.int32)).astype(jnp.float32)
    return 0.54 - 0.46 * jnp.cos(sample_index * (2.0 * math.pi / length))

def cancel_along(extended, time_axis):
    extent = extended.shape[time_axis]
    newest = lax.slice_in_dim(extended, 2, extent, axis=time_axis)
    middle = lax.slice_in_dim(extended, 1, extent - 1, axis=time_axis)
    oldest = lax.slice_in_dim(extended, 0, extent - 2, axis=time_axis)
    return (newest - 2.0 * middle + oldest) * canceller_gain

def reference(image_real, image_imag):
    window = hamming(0, N, N)

    def one_frame(pieces):
        real_part, imag_part = pieces
        padded = jnp.pad(jnp.stack([real_part, imag_part]), ((0, 0), (2, 0), (0, 0)))
        weighted = cancel_along(padded, 1) * window[:, None] * window[None, :]
        spectrum = jnp.fft.fft2(weighted[0] + 1j * weighted[1], norm='ortho')
        return (jnp.transpose(spectrum.real), jnp.transpose(spectrum.imag))
    spectrum_real, spectrum_imag = lax.map(one_frame, (image_real, image_imag))
    return (spectrum_real, spectrum_imag)
```

```python
import math

import jax
import jax.numpy as jnp
from jax import lax
from jax.sharding import PartitionSpec as P

SPLIT_A = 64


canceller_gain = 1.0 / math.sqrt(6.0)


def hamming(offset, sample_count, length):
    sample_index = (offset + jnp.arange(sample_count, dtype=jnp.int32)).astype(jnp.float32)
    return 0.54 - 0.46 * jnp.cos(sample_index * (2.0 * math.pi / length))


def cancel_along(extended, time_axis):
    extent = extended.shape[time_axis]
    newest = lax.slice_in_dim(extended, 2, extent, axis=time_axis)
    middle = lax.slice_in_dim(extended, 1, extent - 1, axis=time_axis)
    oldest = lax.slice_in_dim(extended, 0, extent - 2, axis=time_axis)
    return (newest - 2.0 * middle + oldest) * canceller_gain


def twiddle(row_count, col_count, length):
    product = (
        jnp.arange(row_count, dtype=jnp.int32)[:, None]
        * jnp.arange(col_count, dtype=jnp.int32)[None, :]
        % length
    )
    angles = product.astype(jnp.float32) * (-2.0 * math.pi / length)
    return (jnp.cos(angles), jnp.sin(angles))


def block_matrix(extent):
    cosine_part, sine_part = twiddle(extent, extent, extent)
    return jnp.stack([jnp.stack([cosine_part, -sine_part]), jnp.stack([sine_part, cosine_part])])


def transform_last(stacked, transposed):
    planes, frame_count, middle, length = stacked.shape
    first_size = SPLIT_A
    second_size = length // first_size
    tiled = stacked.reshape(planes, frame_count, middle, first_size, second_size)
    section_one = jnp.einsum(
        "cdki,dfmij->cfmkj",
        block_matrix(first_size),
        tiled,
        precision=lax.Precision.HIGH,
        preferred_element_type=jnp.float32,
    )
    twiddle_real, twiddle_imag = twiddle(first_size, second_size, length)
    turned = jnp.stack(
        [
            section_one[0] * twiddle_real - section_one[1] * twiddle_imag,
            section_one[0] * twiddle_imag + section_one[1] * twiddle_real,
        ]
    )
    if transposed:
        section_two = jnp.einsum(
            "cdlj,dfmkj->cflkm",
            block_matrix(second_size),
            turned,
            precision=lax.Precision.HIGH,
            preferred_element_type=jnp.float32,
        )
        return section_two.reshape(planes, frame_count, length, middle)
    section_two = jnp.einsum(
        "cdlj,dfmkj->cfmlk",
        block_matrix(second_size),
        turned,
        precision=lax.Precision.HIGH,
        preferred_element_type=jnp.float32,
    )
    return section_two.reshape(planes, frame_count, middle, length)


def redistribute(blocks):
    return lax.all_to_all(blocks, "pa", split_axis=0, concat_axis=0, tiled=True)


def first_half(parts, col_window):
    spectrum = transform_last(jnp.stack(parts) * col_window, True)
    planes, frames, length, rows = spectrum.shape
    devices = lax.axis_size("pa")
    blocks = spectrum.reshape(planes, frames, devices, length // devices, rows)
    return jnp.transpose(blocks, (2, 0, 1, 3, 4))


def second_half(blocks, col_window):
    devices, planes, frames, kept, rows = blocks.shape
    length = devices * rows
    columns = jnp.transpose(blocks, (1, 2, 3, 0, 4)).reshape(planes, frames, kept, length)
    padded = jnp.pad(columns, ((0, 0), (0, 0), (0, 0), (2, 0)))
    columns = cancel_along(padded, 3) * col_window
    return transform_last(columns, False) * (1.0 / length)


def body(image_real, image_imag):
    frame_count, row_count, length = image_real.shape
    col_window = hamming(0, length, length)
    pieces = [
        (image_real[frame : frame + 1], image_imag[frame : frame + 1])
        for frame in range(frame_count)
    ]
    ready = first_half(pieces[0], col_window)
    ready, following_piece = lax.optimization_barrier((ready, pieces[min(1, frame_count - 1)]))
    out_real = jnp.zeros((frame_count, length // lax.axis_size("pa"), length), jnp.float32)
    out_imag = jnp.zeros_like(out_real)
    arrived = None
    for frame in range(frame_count):
        moving = redistribute(ready)
        following = ready
        if frame + 1 < frame_count:
            following = first_half(following_piece, col_window)
        if arrived is not None:
            finished = second_half(arrived, col_window)
            out_real = lax.dynamic_update_slice(out_real, finished[0], (frame - 1, 0, 0))
            out_imag = lax.dynamic_update_slice(out_imag, finished[1], (frame - 1, 0, 0))
        arrived, ready, following_piece, out_real, out_imag = lax.optimization_barrier(
            (moving, following, pieces[min(frame + 2, frame_count - 1)], out_real, out_imag)
        )
    finished = second_half(arrived, col_window)
    out_real = lax.dynamic_update_slice(out_real, finished[0], (frame_count - 1, 0, 0))
    out_imag = lax.dynamic_update_slice(out_imag, finished[1], (frame_count - 1, 0, 0))
    return (out_real, out_imag)


def solution(mesh):
    placed = (P(None, "pa", None), P(None, "pa", None))
    return jax.shard_map(
        body,
        mesh=mesh,
        in_specs=placed,
        out_specs=(P(None, "pa", None), P(None, "pa", None)),
        check_vma=False,
    )
```
